512 devices in a mesh: grp: 2 (over y), hist: 16 (over z), chan: 8 (over x), seq: 2 (over core).
Axes of the slice: x: 8, y: 2, z: 16, core: 2. Of those that a mesh axis runs over, the one named last changes fastest.
The devices are a block of a 8x8x16 slice.
Arguments:
- history: bfloat16 [16, 8192, 4096], P(('grp', 'seq'), 'hist', 'chan'), parts along dimension 0, may hold values from -6 to 6
- filter_taps: bfloat16 [16384, 4096], P(('grp', 'hist'), 'chan'), parts along dimension 0, may hold values from -0.0625 to 0.0625
- skip_gain: float32 [8192], P(('grp', 'chan')), parts along dimension 0, may hold values from -4 to 4
- gate_values: bfloat16 [16, 64, 4096], P(('grp', 'seq'), 'hist', 'chan'), parts along dimension 0, may hold values from -6 to 6
Outputs:
- output: bfloat16 [16, 64, 4096], P(('grp', 'seq'), 'hist', 'chan'), parts along dimension 0
The draws below stay inside these ranges and needn't reach their ends.
There are 2 independent parts, one for each index of `grp`. The reference program is written for one: setup_inputs(seed, part) draws one part's arguments, and reference() takes and returns one part's arrays. A program takes and returns all parts, laid end to end along the dimension named above; each array names one. Nothing has to cross between parts.
All inputs are finite; a program needn't handle non-finite values.
Results may differ from the reference program's by a relative error of at most 0.0085.
Values may be sent and summed in bfloat16 or wider, within the bound.
A program may use at most 64 MiB of HBM per device.

```python
import jax
import jax.numpy as jnp
from jax import lax

CH = 4096
SEQS = 8
NEW = 64
TOTAL = 8192


def steps_of(rng, dims, pieces, smallest, top_value):
    def one(axis_at, parts):
        steps = jax.random.uniform(jax.random.fold_in(jax.random.fold_in(rng, 6), axis_at), (parts,), jnp.float32, smallest / len(pieces), top_value / len(pieces))
        return jnp.repeat(jnp.exp(steps), dims[axis_at] // parts).reshape((-1,) + (1,) * (len(dims) - axis_at - 1))

    level = one(*pieces[0])
    for cut in pieces[1:]:
        level = level * one(*cut)
    return level


def scatter_about(rng, shape, spread, reach, pieces=(), dtype=jnp.bfloat16):
    loudness = steps_of(rng, shape, pieces, -0.22, 0.18) if pieces else 1.0
    values = jax.random.normal(rng, shape, jnp.float32) * spread * loudness
    return jnp.minimum(jnp.maximum(values, -reach), reach).astype(dtype)


def setup_inputs(seed: int = 0, part: int = 0) -> dict:
    arg_keys = jax.random.split(jax.random.key(seed), 5)
    part_keys = jax.random.split(jax.random.fold_in(arg_keys[4], part), 5)
    return {
        "history": scatter_about(part_keys[0], (SEQS, TOTAL, CH), 1.0, 6.0, ((0, 2), (1, 16), (2, 8))),
        "filter_taps": scatter_about(part_keys[1], (TOTAL, CH), TOTAL ** -0.5, 0.0625, ((0, 16), (1, 8))),
        "skip_gain": scatter_about(part_keys[2], (CH,), 1.0, 4.0, ((0, 8),), jnp.float32),
        "gate_values": scatter_about(part_keys[3], (SEQS, NEW, CH), 1.0, 6.0, ((0, 2), (1, 16), (2, 8))),
    }


def reference(history, filter_taps, skip_gain, gate_values):
    full_len = history.shape[1]
    fft_len = 2 * full_len
    channels = history.shape[2]
    width = min(256, channels)
    blocks = channels // width
    inputs = history.reshape(history.shape[0], full_len, blocks, width).transpose(2, 0, 1, 3)
    filters = filter_taps[::-1].reshape(full_len, blocks, width).transpose(1, 0, 2)

    def per_block(pair):
        values, taps = pair
        spectrum_in = jnp.fft.rfft(values.astype(jnp.float32), n=fft_len, axis=1)
        spectrum_taps = jnp.fft.rfft(taps.astype(jnp.float32), n=fft_len, axis=0)
        result = jnp.fft.irfft(spectrum_in * spectrum_taps[None], n=fft_len, axis=1)
        return result[:, full_len - NEW:full_len].astype(jnp.float32)

    conv = lax.map(per_block, (inputs, filters))
    conv = conv.transpose(1, 2, 0, 3).reshape(history.shape[0], NEW, channels)
    newest = history[:, full_len - NEW:, :].astype(jnp.float32)
    mixed = conv + skip_gain[None, None, :] * newest
    return (gate_values.astype(jnp.float32) * mixed).astype(jnp.bfloat16)
```

```python
import functools

import jax
import jax.numpy as jnp
import numpy as np
from jax import lax
from jax.experimental import pallas as pl
from jax.experimental.pallas import tpu as pltpu
from jax.sharding import PartitionSpec as P

NEW = 64
BLOCK = 128
LENGTH = BLOCK + NEW
HALF = LENGTH // 2
MESH = pl.DeviceIdType.MESH


def tables():
    freqs = np.arange(HALF) + 0.5
    angle = 2.0 * np.pi / LENGTH * np.outer(freqs, np.arange(LENGTH))
    ahead = np.concatenate([np.cos(angle), np.sin(angle)], axis=0)
    lags = NEW - 1 - np.arange(NEW)
    angle = 2.0 * np.pi / LENGTH * np.outer(lags, freqs)
    back = np.concatenate([np.cos(angle), -np.sin(angle)], axis=1) * (2.0 / LENGTH)
    return jnp.asarray(ahead, jnp.bfloat16), jnp.asarray(back, jnp.bfloat16)


def dot(a, b):
    return jnp.dot(a, b, preferred_element_type=jnp.float32)


def kernel(
    lanes,
    history,
    filter_taps,
    skip_gain,
    ahead,
    back,
    summed,
    hist_buf,
    taps_buf,
    taps_freq,
    data_freq,
    mixed,
    send_buf,
    recv_buf,
    hist_sem,
    taps_sem,
    rim_send,
    rim_recv,
    send_sem,
    recv_sem,
):
    count = lax.axis_size("hist")
    me = lax.axis_index("hist")
    seqs, rows, channels = hist_buf.shape
    tiles = channels // lanes
    groups = rows // BLOCK

    def device(steps):
        return {"hist": lax.rem(me + steps + count, count)}

    taps_copies = [
        pltpu.make_async_copy(
            filter_taps.at[:, pl.ds(t * lanes, lanes)],
            taps_buf.at[pl.ds(0, rows), pl.ds(t * lanes, lanes)],
            taps_sem.at[t],
        )
        for t in range(tiles)
    ]
    hist_copies = [
        [
            pltpu.make_async_copy(
                history.at[b, :, pl.ds(t * lanes, lanes)],
                hist_buf.at[b, :, pl.ds(t * lanes, lanes)],
                hist_sem.at[t, b],
            )
            for b in range(seqs)
        ]
        for t in range(tiles)
    ]
    barrier = pltpu.get_barrier_semaphore()
    for k in range(1, count):
        pl.semaphore_signal(barrier, inc=1, device_id=device(k), device_id_type=MESH)
    for t in range(tiles):
        taps_copies[t].start()
        for b in range(seqs):
            hist_copies[t][b].start()

    rims = [
        pltpu.make_async_remote_copy(
            src_ref=taps_buf.at[pl.ds(0, NEW), pl.ds(t * lanes, lanes)],
            dst_ref=taps_buf.at[pl.ds(rows, NEW), pl.ds(t * lanes, lanes)],
            send_sem=rim_send.at[t],
            recv_sem=rim_recv.at[t],
            device_id=device(-1),
            device_id_type=MESH,
        )
        for t in range(tiles)
    ]
    for t in range(tiles):
        taps_copies[t].wait()
    pl.semaphore_wait(barrier, count - 1)
    for t in range(tiles):
        rims[t].start()

    sends = []
    is_last = me == count - 1
    last_flag = is_last.astype(jnp.float32)
    row_ids = lax.broadcasted_iota(jnp.int32, (NEW, lanes), 0)
    low = lax.rem(row_ids, 8) < 4
    for t in range(tiles):
        cols = pl.ds(t * lanes, lanes)
        rims[t].wait_recv()
        for g in range(groups):
            if g == groups - 1:
                rim = taps_buf[pl.ds(rows, NEW), cols]
                rim = jnp.where(is_last, jnp.zeros_like(rim), rim)
                taps = jnp.concatenate([taps_buf[pl.ds(g * BLOCK, BLOCK), cols], rim], axis=0)
            else:
                taps = taps_buf[pl.ds(g * BLOCK, LENGTH), cols]
            taps_freq[g] = dot(ahead[...], taps)
        partial = []
        for b in range(seqs):
            hist_copies[t][b].wait()
            for g in range(groups):
                data_freq[g] = dot(ahead[:, :BLOCK], hist_buf[b, pl.ds(g * BLOCK, BLOCK), cols])
            for r in range(0, HALF, 16):
                real = imag = None
                for g in range(groups):
                    tc = taps_freq[g, pl.ds(r, 16), :]
                    ts = taps_freq[g, pl.ds(HALF + r, 16), :]
                    dc = data_freq[g, pl.ds(r, 16), :]
                    ds = data_freq[g, pl.ds(HALF + r, 16), :]
                    re = tc * dc + ts * ds
                    im = tc * ds - ts * dc
                    real = re if real is None else real + re
                    imag = im if imag is None else imag + im
                mixed[pl.ds(r, 16), :] = real.astype(jnp.bfloat16)
                mixed[pl.ds(HALF + r, 16), :] = imag.astype(jnp.bfloat16)
            value = dot(back[...], mixed[...])
            newest = hist_buf[b, pl.ds(rows - NEW, NEW), cols].astype(jnp.float32)
            partial.append(value + (last_flag * skip_gain[:, cols]) * newest)
        evens, odds = [], []
        for b in range(0, seqs, 2):
            first, second = partial[b], partial[b + 1]
            evens.append(jnp.where(low, first, pltpu.roll(second, 4, 0)))
            odds.append(jnp.where(low, pltpu.roll(first, NEW - 4, 0), second))
        for d in range(count):
            source = odds if d % 2 else evens
            at = d // 2 * 8
            piece = jnp.concatenate([source[0][at : at + 8], source[1][at : at + 8]], axis=0)
            send_buf[t, d] = piece.astype(jnp.bfloat16)
        for k in range(1, count):
            owner = lax.rem(me + k, count)
            copy = pltpu.make_async_remote_copy(
                src_ref=send_buf.at[t, owner],
                dst_ref=recv_buf.at[t, k],
                send_sem=send_sem.at[t, k],
                recv_sem=recv_sem.at[t, k],
                device_id=device(k),
                device_id_type=MESH,
            )
            copy.start()
            sends.append(copy)
    for t in range(tiles):
        total = send_buf[t, me].astype(jnp.float32)
        for k in range(1, count):
            sends[t * (count - 1) + k - 1].wait_recv()
            total = total + recv_buf[t, k].astype(jnp.float32)
        summed[:, pl.ds(t * lanes, lanes)] = total
    for t in range(tiles):
        rims[t].wait_send()
    for copy in sends:
        copy.wait_send()


def body(history, filter_taps, skip_gain, gate_values):
    count = lax.axis_size("hist")
    seqs, rows, channels = history.shape
    own = gate_values.shape[1]
    lanes = min(256, channels)
    tiles = channels // lanes
    groups = rows // BLOCK
    ahead, back = tables()
    anywhere = pl.BlockSpec(memory_space=pl.ANY)
    vmem = pl.BlockSpec(memory_space=pltpu.VMEM)
    summed = pl.pallas_call(
        functools.partial(kernel, lanes),
        out_shape=jax.ShapeDtypeStruct((seqs * own, channels), jnp.float32),
        in_specs=[anywhere, anywhere, vmem, vmem, vmem],
        out_specs=vmem,
        scratch_shapes=[
            pltpu.VMEM((seqs, rows, channels), jnp.bfloat16),
            pltpu.VMEM((rows + NEW, channels), jnp.bfloat16),
            pltpu.VMEM((groups, LENGTH, lanes), jnp.float32),
            pltpu.VMEM((groups, LENGTH, lanes), jnp.float32),
            pltpu.VMEM((LENGTH, lanes), jnp.bfloat16),
            pltpu.VMEM((tiles, count, seqs * own, lanes), jnp.bfloat16),
            pltpu.VMEM((tiles, count, seqs * own, lanes), jnp.bfloat16),
            pltpu.SemaphoreType.DMA((tiles, seqs)),
            pltpu.SemaphoreType.DMA((tiles,)),
            pltpu.SemaphoreType.DMA((tiles,)),
            pltpu.SemaphoreType.DMA((tiles,)),
            pltpu.SemaphoreType.DMA((tiles, count)),
            pltpu.SemaphoreType.DMA((tiles, count)),
        ],
        compiler_params=pltpu.CompilerParams(collective_id=0, has_side_effects=True),
        name="hyena_window",
    )(history, filter_taps, skip_gain.reshape(1, channels), ahead, back)
    return (gate_values.astype(jnp.float32) * summed.reshape(seqs, own, channels)).astype(jnp.bfloat16)


def solution(mesh):
    placed = (
        P(("grp", "seq"), "hist", "chan"),
        P(("grp", "hist"), "chan"),
        P(("grp", "chan")),
        P(("grp", "seq"), "hist", "chan"),
    )
    return jax.shard_map(
        body,
        mesh=mesh,
        in_specs=placed,
        out_specs=P(("grp", "seq"), "hist", "chan"),
        check_vma=False,
    )
```

```python
import functools

import jax
import jax.numpy as jnp
import numpy as np
from jax import lax
from jax.experimental import pallas as pl
from jax.experimental.pallas import tpu as pltpu
from jax.sharding import PartitionSpec as P

NEW = 64
BLOCK = 128
LENGTH = BLOCK + NEW
HALF = LENGTH // 2
STEP = 16
MESH = pl.DeviceIdType.MESH


def tables():
    freqs = np.arange(HALF) + 0.5
    angle = 2.0 * np.pi / LENGTH * np.outer(freqs, np.arange(LENGTH))
    ahead = np.concatenate([np.cos(angle), np.sin(angle)], axis=0)
    lags = NEW - 1 - np.arange(NEW)
    angle = 2.0 * np.pi / LENGTH * np.outer(lags, freqs)
    back = np.concatenate([np.cos(angle), -np.sin(angle)], axis=1) * (2.0 / LENGTH)
    return jnp.asarray(ahead, jnp.bfloat16), jnp.asarray(back, jnp.bfloat16)


def dot(a, b):
    return jnp.dot(a, b, preferred_element_type=jnp.float32)


def kernel(
    lanes,
    history,
    filter_taps,
    skip_gain,
    gate_values,
    ahead_table,
    back_table,
    output,
    hist_buf,
    taps_buf,
    skip_buf,
    gate_buf,
    ahead,
    back,
    taps_freq,
    data_freq,
    last_freq,
    mixed,
    partial,
    send_buf,
    recv_buf,
    hist_sem,
    taps_sem,
    head_sem,
    small_sem,
    rim_send,
    rim_recv,
    send_sem,
    recv_sem,
    ready_sem,
):
    count = lax.axis_size("hist")
    me = lax.axis_index("hist")
    seqs, rows, channels = hist_buf.shape
    own = NEW // count
    tiles = channels // lanes
    groups = rows // BLOCK
    last = count - 1

    late = max(count - 3, 1)
    order = list(range(1, late)) + [0] + list(range(late, count))
    place = jnp.where(me == 0, late - 1, jnp.where(me < late, me - 1, me))

    def cols(t):
        return pl.ds(t * lanes, lanes)

    heads = [
        pltpu.make_async_copy(
            filter_taps.at[pl.ds(0, NEW), cols(t)],
            taps_buf.at[pl.ds(0, NEW), cols(t)],
            head_sem.at[t],
        )
        for t in range(tiles)
    ]
    taps_copies = [
        pltpu.make_async_copy(
            filter_taps.at[pl.ds(NEW, rows - NEW), cols(t)],
            taps_buf.at[pl.ds(NEW, rows - NEW), cols(t)],
            taps_sem.at[t],
        )
        for t in range(tiles)
    ]
    hist_copies = [
        [
            pltpu.make_async_copy(
                history.at[b, :, cols(t)], hist_buf.at[b, :, cols(t)], hist_sem.at[t, b]
            )
            for b in range(seqs)
        ]
        for t in range(tiles)
    ]
    smalls = [
        pltpu.make_async_copy(source, target, small_sem.at[i])
        for i, (source, target) in enumerate(
            [
                (ahead_table, ahead),
                (back_table, back),
                (skip_gain, skip_buf),
                (gate_values, gate_buf),
            ]
        )
    ]
    for copy in heads:
        copy.start()
    smalls[0].start()
    for t in range(tiles):
        taps_copies[t].start()
        for b in range(seqs):
            hist_copies[t][b].start()
    for copy in smalls[1:]:
        copy.start()

    barrier = pltpu.get_barrier_semaphore()
    for spot, other in enumerate(order):

        @pl.when(place < spot)
        def _():
            pl.semaphore_signal(barrier, inc=1, device_id={"hist": other}, device_id_type=MESH)

    def rim(t):
        return pltpu.make_async_remote_copy(
            src_ref=taps_buf.at[pl.ds(0, NEW), cols(t)],
            dst_ref=taps_buf.at[pl.ds(rows, NEW), cols(t)],
            send_sem=rim_send.at[t],
            recv_sem=rim_recv.at[t],
            device_id={"hist": lax.rem(me + last, count)},
            device_id_type=MESH,
        )

    def main_part(t):
        taps_copies[t].wait()
        for g in range(groups):
            span = BLOCK if g == groups - 1 else LENGTH
            taps_freq[g] = dot(ahead[:, :span], taps_buf[pl.ds(g * BLOCK, span), cols(t)])
        for b in range(seqs):
            hist_copies[t][b].wait()
            for g in range(groups):
                freq = dot(ahead[:, :BLOCK], hist_buf[b, pl.ds(g * BLOCK, BLOCK), cols(t)])
                if g == groups - 1:
                    last_freq[t, b] = freq
                else:
                    data_freq[g] = freq
            for r in range(0, HALF, STEP):
                real = imag = None
                upper, lower = pl.ds(r, STEP), pl.ds(HALF + r, STEP)
                for g in range(groups):
                    data = last_freq.at[t, b] if g == groups - 1 else data_freq.at[g]
                    tc, ts = taps_freq[g, upper, :], taps_freq[g, lower, :]
                    dc, ds = data[upper, :], data[lower, :]
                    re = tc * dc + ts * ds
                    im = tc * ds - ts * dc
                    real = re if real is None else real + re
                    imag = im if imag is None else imag + im
                mixed[upper, :] = real.astype(jnp.bfloat16)
                mixed[lower, :] = imag.astype(jnp.bfloat16)
            partial[t, b] = dot(back[...], mixed[...])

    def corner_part(t):
        taps_freq[0] = dot(ahead[:, BLOCK:], taps_buf[pl.ds(rows, NEW), cols(t)])
        for b in range(seqs):
            for r in range(0, HALF, STEP):
                upper, lower = pl.ds(r, STEP), pl.ds(HALF + r, STEP)
                tc, ts = taps_freq[0, upper, :], taps_freq[0, lower, :]
                dc, ds = last_freq[t, b, upper, :], last_freq[t, b, lower, :]
                mixed[upper, :] = (tc * dc + ts * ds).astype(jnp.bfloat16)
                mixed[lower, :] = (tc * ds - ts * dc).astype(jnp.bfloat16)
            partial[t, b] += dot(back[...], mixed[...])

    def skip_part(t):
        for b in range(seqs):
            newest = hist_buf[b, pl.ds(rows - NEW, NEW), cols(t)].astype(jnp.float32)
            partial[t, b] += skip_buf[:, cols(t)] * newest

    def pack(t):
        low = lax.rem(lax.broadcasted_iota(jnp.int32, (NEW, lanes), 0), 8) < 4
        evens, odds = [], []
        for b in range(0, seqs, 2):
            first, second = partial[t, b], partial[t, b + 1]
            evens.append(jnp.where(low, first, pltpu.roll(second, 4, 0)))
            odds.append(jnp.where(low, pltpu.roll(first, NEW - 4, 0), second))
        for d in range(count):
            source = odds if d % 2 else evens
            at = d // 2 * 8
            piece = jnp.concatenate([source[0][at : at + 8], source[1][at : at + 8]], axis=0)
            send_buf[d, :, cols(t)] = piece.astype(jnp.bfloat16)

    def send(d):
        return pltpu.make_async_remote_copy(
            src_ref=send_buf.at[d],
            dst_ref=recv_buf.at[me],
            send_sem=send_sem.at[d],
            recv_sem=recv_sem.at[me],
            device_id={"hist": d},
            device_id_type=MESH,
        )

    def arrival(d):
        return pltpu.make_async_remote_copy(
            src_ref=send_buf.at[d],
            dst_ref=recv_buf.at[d],
            send_sem=send_sem.at[d],
            recv_sem=recv_sem.at[d],
            device_id={"hist": d},
            device_id_type=MESH,
        )

    for copy in heads:
        copy.wait()

    def meet():
        @pl.when(place > 0)
        def _():
            pl.semaphore_wait(barrier, place)

        @pl.when(me > 1)
        def _():
            for t in range(tiles):
                rim(t).start()

        for spot, other in enumerate(order):

            @pl.when(spot < place)
            def _():
                pl.semaphore_signal(
                    ready_sem.at[me], inc=1, device_id={"hist": other}, device_id_type=MESH
                )

    @pl.when(me >= late)
    def _():
        meet()

    for copy in smalls:
        copy.wait()
    for t in range(tiles):
        main_part(t)

    @pl.when(me < late)
    def _():
        meet()

    @pl.when(me != last)
    def _():
        for t in range(tiles):
            rim(t).wait_recv()
            corner_part(t)

    @pl.when(me == last)
    def _():
        for t in range(tiles):
            skip_part(t)

    for t in range(tiles):
        pack(t)

    @pl.when(me >= late)
    def _():
        send(0).start()

    for spot, d in enumerate(order):

        @pl.when(place < spot)
        def _():
            pl.semaphore_wait(ready_sem.at[d], 1)

        if d == 0:

            @pl.when(me == 1)
            def _():
                for t in range(tiles):
                    rim(t).start()

            @pl.when(jnp.logical_and(me != 0, me < late))
            def _():
                send(0).start()

        else:

            @pl.when(me != d)
            def _():
                send(d).start()

    gate = jnp.concatenate([gate_buf[b].astype(jnp.float32) for b in range(seqs)], axis=0)
    recv_buf[me] = send_buf[me]
    total = None
    for d in range(count):

        @pl.when(me != d)
        def _():
            arrival(d).wait_recv()

        value = recv_buf[d].astype(jnp.float32)
        total = value if total is None else total + value
    result = (gate * total).astype(jnp.bfloat16)
    for b in range(seqs):
        output[b] = result[b * own : (b + 1) * own]

    @pl.when(me > 0)
    def _():
        for t in range(tiles):
            rim(t).wait_send()

    for d in range(count):

        @pl.when(me != d)
        def _():
            send(d).wait_send()


def body(history, filter_taps, skip_gain, gate_values):
    count = lax.axis_size("hist")
    seqs, rows, channels = history.shape
    own = gate_values.shape[1]
    lanes = min(256, channels)
    tiles = channels // lanes
    groups = rows // BLOCK
    ahead, back = tables()
    anywhere = pl.BlockSpec(memory_space=pl.ANY)
    f32, bf16 = jnp.float32, jnp.bfloat16
    return pl.pallas_call(
        functools.partial(kernel, lanes),
        out_shape=jax.ShapeDtypeStruct((seqs, own, channels), bf16),
        in_specs=[anywhere] * 6,
        out_specs=pl.BlockSpec(memory_space=pltpu.VMEM),
        scratch_shapes=[
            pltpu.VMEM((seqs, rows, channels), bf16),
            pltpu.VMEM((rows + NEW, channels), bf16),
            pltpu.VMEM((1, channels), f32),
            pltpu.VMEM((seqs, own, channels), bf16),
            pltpu.VMEM(ahead.shape, bf16),
            pltpu.VMEM(back.shape, bf16),
            pltpu.VMEM((groups, LENGTH, lanes), f32),
            pltpu.VMEM((groups - 1, LENGTH, lanes), f32),
            pltpu.VMEM((tiles, seqs, LENGTH, lanes), f32),
            pltpu.VMEM((LENGTH, lanes), bf16),
            pltpu.VMEM((tiles, seqs, NEW, lanes), f32),
            pltpu.VMEM((count, seqs * own, channels), bf16),
            pltpu.VMEM((count, seqs * own, channels), bf16),
            pltpu.SemaphoreType.DMA((tiles, seqs)),
            pltpu.SemaphoreType.DMA((tiles,)),
            pltpu.SemaphoreType.DMA((tiles,)),
            pltpu.SemaphoreType.DMA((4,)),
            pltpu.SemaphoreType.DMA((tiles,)),
            pltpu.SemaphoreType.DMA((tiles,)),
            pltpu.SemaphoreType.DMA((count,)),
            pltpu.SemaphoreType.DMA((count,)),
            pltpu.SemaphoreType.REGULAR((count,)),
        ],
        compiler_params=pltpu.CompilerParams(collective_id=0, has_side_effects=True),
        name="hyena_window",
    )(history, filter_taps, skip_gain.reshape(1, channels), gate_values, ahead, back)


def solution(mesh):
    placed = (
        P(("grp", "seq"), "hist", "chan"),
        P(("grp", "hist"), "chan"),
        P(("grp", "chan")),
        P(("grp", "seq"), "hist", "chan"),
    )
    return jax.shard_map(
        body,
        mesh=mesh,
        in_specs=placed,
        out_specs=P(("grp", "seq"), "hist", "chan"),
        check_vma=False,
    )
```

```python
import functools

import jax
import jax.numpy as jnp
import numpy as np
from jax import lax
from jax.experimental import pallas as pl
from jax.experimental.pallas import tpu as pltpu
from jax.sharding import PartitionSpec as P

NEW = 64
BLOCK = 128
LENGTH = BLOCK + NEW
HALF = LENGTH // 2
STEP = 16
LOWER = HALF + 8
PADDED = LOWER + HALF
MESH = pl.DeviceIdType.MESH


def tables():
    freqs = np.arange(HALF) + 0.5
    angle = 2.0 * np.pi / LENGTH * np.outer(freqs, np.arange(LENGTH))
    ahead = np.concatenate([np.cos(angle), np.sin(angle)], axis=0)
    lags = NEW - 1 - np.arange(NEW)
    angle = 2.0 * np.pi / LENGTH * np.outer(lags, freqs)
    back = np.concatenate([np.cos(angle), -np.sin(angle)], axis=1) * (2.0 / LENGTH)
    return jnp.asarray(ahead, jnp.bfloat16), jnp.asarray(back, jnp.bfloat16)


def dot(a, b):
    return jnp.dot(a, b, preferred_element_type=jnp.float32)


def kernel(
    lanes,
    history,
    filter_taps,
    skip_gain,
    gate_values,
    ahead_table,
    back_table,
    output,
    hist_buf,
    taps_buf,
    ahead,
    back,
    taps_freq,
    data_freq,
    last_freq,
    mixed,
    partial,
    send_buf,
    recv_buf,
    gate_buf,
    skip_buf,
    hist_sem,
    taps_sem,
    small_sem,
    rim_send,
    rim_recv,
    send_sem,
    recv_sem,
    ready_sem,
    zero_sem,
):
    count = lax.axis_size("hist")
    me = lax.axis_index("hist")
    seqs, rows, channels = hist_buf.shape
    own = NEW // count
    tiles = channels // lanes
    groups = rows // BLOCK
    last = count - 1

    beside = [i for i in range(1, count) if i <= 3 or i >= count - 3]
    relays = {i: 3 if i < 8 else 7 if i < 12 else 1 for i in range(1, count) if i not in beside}
    tail = range(count - 3, count)

    def is_in(group):
        found = me == group[0]
        for i in group[1:]:
            found = jnp.logical_or(found, me == i)
        return found

    is_beside = is_in(beside)

    def cols(t):
        if not isinstance(t, int):
            return pl.ds(pl.multiple_of(t * lanes, lanes), lanes)
        return pl.ds(t * lanes, lanes)

    def taps_copy(t):
        return pltpu.make_async_copy(
            filter_taps.at[:, cols(t)], taps_buf.at[pl.ds(0, rows), cols(t)], taps_sem.at[t]
        )

    def hist_copy(t, b):
        return pltpu.make_async_copy(
            history.at[b, :, cols(t)], hist_buf.at[b, :, cols(t)], hist_sem.at[t, b]
        )

    smalls = [
        pltpu.make_async_copy(source, target, small_sem.at[i])
        for i, (source, target) in enumerate(
            [
                (ahead_table, ahead),
                (back_table, back),
                (skip_gain, skip_buf),
                (gate_values, gate_buf),
            ]
        )
    ]
    barrier = pltpu.get_barrier_semaphore()

    def rim(t):
        return pltpu.make_async_remote_copy(
            src_ref=filter_taps.at[pl.ds(0, NEW), cols(t)],
            dst_ref=taps_buf.at[pl.ds(rows, NEW), cols(t)],
            send_sem=rim_send.at[t],
            recv_sem=rim_recv.at[t],
            device_id={"hist": lax.rem(me + last, count)},
            device_id_type=MESH,
        )

    def keep(ref, freq):
        ref[:HALF, :] = freq[:HALF]
        ref[LOWER:, :] = freq[HALF:]

    def main_part(t):
        taps_copy(t).wait()
        for g in range(groups):
            span = BLOCK if g == groups - 1 else LENGTH
            keep(taps_freq.at[g], dot(ahead[:, :span], taps_buf[pl.ds(g * BLOCK, span), cols(t)]))
        for b in range(seqs):
            hist_copy(t, b).wait()
            for g in range(groups):
                freq = dot(ahead[:, :BLOCK], hist_buf[b, pl.ds(g * BLOCK, BLOCK), cols(t)])
                if g == groups - 1:
                    keep(last_freq.at[t, b], freq)
                else:
                    keep(data_freq.at[b % 2, g], freq)
            for r in range(0, HALF, STEP):
                real = imag = None
                upper, lower, under = pl.ds(r, STEP), pl.ds(LOWER + r, STEP), pl.ds(HALF + r, STEP)
                for g in range(groups):
                    data = last_freq.at[t, b] if g == groups - 1 else data_freq.at[b % 2, g]
                    tc, ts = taps_freq[g, upper, :], taps_freq[g, lower, :]
                    dc, ds = data[upper, :], data[lower, :]
                    re = tc * dc + ts * ds
                    im = tc * ds - ts * dc
                    real = re if real is None else real + re
                    imag = im if imag is None else imag + im
                mixed[b % 2, upper, :] = real.astype(jnp.bfloat16)
                mixed[b % 2, under, :] = imag.astype(jnp.bfloat16)
            partial[t, b] = dot(back[...], mixed[b % 2])

    def corner_part(t):
        keep(taps_freq.at[0], dot(ahead[:, BLOCK:], taps_buf[pl.ds(rows, NEW), cols(t)]))
        for b in range(seqs):
            for r in range(0, HALF, STEP):
                upper, lower, under = pl.ds(r, STEP), pl.ds(LOWER + r, STEP), pl.ds(HALF + r, STEP)
                tc, ts = taps_freq[0, upper, :], taps_freq[0, lower, :]
                dc, ds = last_freq[t, b, upper, :], last_freq[t, b, lower, :]
                mixed[b % 2, upper, :] = (tc * dc + ts * ds).astype(jnp.bfloat16)
                mixed[b % 2, under, :] = (tc * ds - ts * dc).astype(jnp.bfloat16)
            partial[t, b] += dot(back[...], mixed[b % 2])

    def skip_part(t):
        for b in range(seqs):
            newest = hist_buf[b, pl.ds(rows - NEW, NEW), cols(t)].astype(jnp.float32)
            partial[t, b] += skip_buf[:, cols(t)] * newest

    def pack(t):
        low = lax.rem(lax.broadcasted_iota(jnp.int32, (NEW, lanes), 0), 8) < 4
        evens, odds = [], []
        for b in range(0, seqs, 2):
            first, second = partial[t, b], partial[t, b + 1]
            evens.append(jnp.where(low, first, pltpu.roll(second, 4, 0)))
            odds.append(jnp.where(low, pltpu.roll(first, NEW - 4, 0), second))
        for d in range(count):
            source = odds if d % 2 else evens
            at = d // 2 * 8
            piece = jnp.concatenate([source[0][at : at + 8], source[1][at : at + 8]], axis=0)
            send_buf[d, :, cols(t)] = piece.astype(jnp.bfloat16)

    def send(d):
        return pltpu.make_async_remote_copy(
            src_ref=send_buf.at[d],
            dst_ref=recv_buf.at[me],
            send_sem=send_sem.at[d],
            recv_sem=recv_sem.at[me],
            device_id={"hist": d},
            device_id_type=MESH,
        )

    def arrival(d):
        return pltpu.make_async_remote_copy(
            src_ref=send_buf.at[d],
            dst_ref=recv_buf.at[d],
            send_sem=send_sem.at[d],
            recv_sem=recv_sem.at[d],
            device_id={"hist": d},
            device_id_type=MESH,
        )

    def greet():
        for other in range(1, count):
            told = jnp.logical_and(me > 0, me < other)
            if other in beside:
                told = me < other

            @pl.when(told)
            def _():
                pl.semaphore_signal(barrier, inc=1, device_id={"hist": other}, device_id_type=MESH)

    def tell_ready(other):
        pl.semaphore_signal(
            ready_sem.at[me], inc=1, device_id={"hist": other}, device_id_type=MESH
        )

    def meet():
        pl.semaphore_wait(barrier, me - jnp.where(is_beside, 0, 1))
        for t in range(tiles):
            rim(t).start()

        @pl.when(is_beside)
        def _():
            tell_ready(0)

        for other in range(1, count - 1):

            @pl.when(other < me)
            def _():
                tell_ready(other)

    smalls[0].start()
    smalls[1].start()
    taps_copy(0).start()
    for b in range(seqs // 2):
        hist_copy(0, b).start()

    with jax.named_scope("greet"):
        greet()

    with jax.named_scope("meet"):

        @pl.when(me != 0)
        def _():
            meet()

    with jax.named_scope("loads"):
        for b in range(seqs // 2, seqs):
            hist_copy(0, b).start()
        for t in range(1, tiles):
            taps_copy(t).start()
            for b in range(seqs):
                hist_copy(t, b).start()
        for copy in smalls[2:]:
            copy.start()

    with jax.named_scope("ahead"):
        smalls[0].wait()
        smalls[1].wait()
    @pl.loop(0, tiles)
    def _(t):
        with jax.named_scope("main"):
            main_part(t)

    @pl.when(me != last)
    def _():
        @pl.loop(0, tiles)
        def _(t):
            with jax.named_scope("rim_wait"):
                rim(t).wait_recv()
            with jax.named_scope("corner"):
                corner_part(t)

    with jax.named_scope("skip"):
        smalls[2].wait()
        smalls[3].wait()

        @pl.when(me == last)
        def _():
            for t in range(tiles):
                skip_part(t)

    with jax.named_scope("pack"):
        for t in range(tiles):
            pack(t)

    def ready(d):
        with jax.named_scope("ready"):

            @pl.when(me < d)
            def _():
                pl.semaphore_wait(ready_sem.at[d], 1)

    def relay(d):
        if d in relays:

            @pl.when(me == relays[d])
            def _():
                pl.semaphore_signal(zero_sem, inc=1, device_id={"hist": d}, device_id_type=MESH)

    is_late = me >= count - 2
    singly = 2

    @pl.when(is_beside)
    def _():
        send(0).start()

    @pl.when(is_late)
    def _():
        send(0).wait_send()

    is_between = jnp.logical_not(jnp.logical_or(is_beside, me == 0))

    @pl.when(is_between)
    def _():
        for d in range(1, 4):
            send(d).start()

    with jax.named_scope("zero"):

        @pl.when(is_between)
        def _():
            pl.semaphore_wait(zero_sem, 1)
            tell_ready(0)
            send(0).start()

    for d in range(1, count):
        if d in tail:
            now = jnp.logical_or(me == 0, me > d)

            @pl.when(now)
            def _():
                ready(d)

        else:
            now = me != d
            if d < 4:
                now = jnp.logical_and(now, jnp.logical_not(is_between))
            ready(d)
            relay(d)

        @pl.when(now)
        def _():
            send(d).start()

        if d < singly:

            @pl.when(is_late)
            def _():
                send(d).wait_send()

    def arrive(d):
        with jax.named_scope("arrive"):

            @pl.when(me != d)
            def _():
                arrival(d).wait_recv()

    arrive(last - 2)
    for d in tail:

        @pl.when(jnp.logical_and(me > 0, me < d))
        def _():
            ready(d)
            send(d).start()

    gate = jnp.concatenate([gate_buf[b].astype(jnp.float32) for b in range(seqs)], axis=0)
    recv_buf[me] = send_buf[me]
    total = None
    for d in range(count):
        if d != last - 2:
            arrive(d)
        value = recv_buf[d].astype(jnp.float32)
        total = value if total is None else total + value
    result = (gate * total).astype(jnp.bfloat16)
    for b in range(seqs):
        output[b] = result[b * own : (b + 1) * own]

    with jax.named_scope("drain"):

        @pl.when(me > 0)
        def _():
            for t in range(tiles):
                rim(t).wait_send()

        for d in range(count):
            left = me != d
            if d < singly:
                left = jnp.logical_and(left, jnp.logical_not(is_late))

            @pl.when(left)
            def _():
                send(d).wait_send()


def body(history, filter_taps, skip_gain, gate_values):
    count = lax.axis_size("hist")
    seqs, rows, channels = history.shape
    own = gate_values.shape[1]
    lanes = min(256, channels)
    tiles = channels // lanes
    groups = rows // BLOCK
    ahead, back = tables()
    anywhere = pl.BlockSpec(memory_space=pl.ANY)
    f32, bf16 = jnp.float32, jnp.bfloat16
    return pl.pallas_call(
        functools.partial(kernel, lanes),
        out_shape=pltpu.VMEM((seqs, own, channels), bf16),
        in_specs=[anywhere] * 6,
        out_specs=pl.BlockSpec(memory_space=pltpu.VMEM),
        scratch_shapes=[
            pltpu.VMEM((seqs, rows, channels), bf16),
            pltpu.VMEM((rows + NEW, channels), bf16),
            pltpu.VMEM(ahead.shape, bf16),
            pltpu.VMEM(back.shape, bf16),
            pltpu.VMEM((groups, PADDED, lanes), f32),
            pltpu.VMEM((2, groups - 1, PADDED, lanes), f32),
            pltpu.VMEM((tiles, seqs, PADDED, lanes), f32),
            pltpu.VMEM((2, LENGTH, lanes), bf16),
            pltpu.VMEM((tiles, seqs, NEW, lanes), f32),
            pltpu.VMEM((count, seqs * own, channels), bf16),
            pltpu.VMEM((count, seqs * own, channels), bf16),
            pltpu.VMEM((seqs, own, channels), bf16),
            pltpu.VMEM((1, channels), f32),
            pltpu.SemaphoreType.DMA((tiles, seqs)),
            pltpu.SemaphoreType.DMA((tiles,)),
            pltpu.SemaphoreType.DMA((4,)),
            pltpu.SemaphoreType.DMA((tiles,)),
            pltpu.SemaphoreType.DMA((tiles,)),
            pltpu.SemaphoreType.DMA((count,)),
            pltpu.SemaphoreType.DMA((count,)),
            pltpu.SemaphoreType.REGULAR((count,)),
            pltpu.SemaphoreType.REGULAR,
        ],
        compiler_params=pltpu.CompilerParams(collective_id=0, has_side_effects=True),
        name="hyena_window",
    )(history, filter_taps, skip_gain.reshape(1, channels), gate_values, ahead, back)


def solution(mesh):
    placed = (
        P(("grp", "seq"), "hist", "chan"),
        P(("grp", "hist"), "chan"),
        P(("grp", "chan")),
        P(("grp", "seq"), "hist", "chan"),
    )
    return jax.shard_map(
        body,
        mesh=mesh,
        in_specs=placed,
        out_specs=P(("grp", "seq"), "hist", "chan"),
        check_vma=False,
    )
```

```python
import functools

import jax
import jax.numpy as jnp
import numpy as np
from jax import lax
from jax.experimental import pallas as pl
from jax.experimental.pallas import tpu as pltpu
from jax.sharding import PartitionSpec as P

NEW = 64
BLOCK = 128
LENGTH = BLOCK + NEW
HALF = LENGTH // 2
STEP = 16
MESH = pl.DeviceIdType.MESH


def tables():
    freqs = np.arange(HALF) + 0.5
    angle = 2.0 * np.pi / LENGTH * np.outer(freqs, np.arange(LENGTH))
    ahead = np.concatenate([np.cos(angle), np.sin(angle)], axis=0)
    lags = NEW - 1 - np.arange(NEW)
    angle = 2.0 * np.pi / LENGTH * np.outer(lags, freqs)
    back = np.concatenate([np.cos(angle), -np.sin(angle)], axis=1) * (2.0 / LENGTH)
    return jnp.asarray(ahead, jnp.bfloat16), jnp.asarray(back, jnp.bfloat16)


def dot(a, b):
    return jnp.dot(a, b, preferred_element_type=jnp.float32)


def kernel(
    lanes,
    parts,
    history,
    filter_taps,
    skip_gain,
    gate_values,
    ahead_table,
    back_table,
    output,
    hist_buf,
    taps_buf,
    ahead,
    back,
    taps_freq,
    data_freq,
    last_freq,
    mixed,
    partial,
    send_buf,
    recv_buf,
    gate_buf,
    skip_buf,
    hist_sem,
    taps_sem,
    small_sem,
    rim_send,
    rim_recv,
    send_sem,
    recv_sem,
    ready_sem,
    zero_sem,
):
    count = lax.axis_size("hist")
    me = lax.axis_index("hist")
    seqs, rows, channels = hist_buf.shape
    own = NEW // count
    tiles = channels // lanes
    groups = rows // BLOCK
    last = count - 1

    beside = [i for i in range(1, count) if i <= 3 or i >= count - 3]
    relays = {i: 3 if i < 8 else 7 if i < 12 else 1 for i in range(1, count) if i not in beside}
    tail = range(count - 3, count)

    def is_in(group):
        found = me == group[0]
        for i in group[1:]:
            found = jnp.logical_or(found, me == i)
        return found

    is_beside = is_in(beside)

    def cols(t):
        if not isinstance(t, int):
            return pl.ds(pl.multiple_of(t * lanes, lanes), lanes)
        return pl.ds(t * lanes, lanes)

    def taps_copy(t):
        return pltpu.make_async_copy(
            filter_taps.at[:, cols(t)], taps_buf.at[pl.ds(0, rows), cols(t)], taps_sem.at[t]
        )

    def hist_copy(t, b):
        return pltpu.make_async_copy(
            history.at[b, :, cols(t)], hist_buf.at[b, :, cols(t)], hist_sem.at[t, b]
        )

    smalls = [
        pltpu.make_async_copy(source, target, small_sem.at[i])
        for i, (source, target) in enumerate(
            [
                (ahead_table, ahead),
                (back_table, back),
                (skip_gain, skip_buf),
                (gate_values, gate_buf),
            ]
        )
    ]
    barrier = pltpu.get_barrier_semaphore()

    cores = lax.axis_size("seq")
    core = lax.axis_index("seq")
    sender = cores - 1
    width = channels // parts

    def rim(p, target):
        lane = pl.ds(p * width, width)
        return pltpu.make_async_remote_copy(
            src_ref=filter_taps.at[pl.ds(0, NEW), lane],
            dst_ref=taps_buf.at[pl.ds(rows, NEW), lane],
            send_sem=rim_send.at[p, target],
            recv_sem=rim_recv.at[p],
            device_id={"hist": lax.rem(me + last, count), "seq": target},
            device_id_type=MESH,
        )

    def sends_rim(target):
        return jnp.where(me > 1, core == sender, jnp.logical_and(me == 1, core == target))

    def main_part(t):
        taps_copy(t).wait()
        for g in range(groups):
            span = BLOCK if g == groups - 1 else LENGTH
            taps_freq[g] = dot(ahead[:, :span], taps_buf[pl.ds(g * BLOCK, span), cols(t)])
        for b in range(seqs):
            hist_copy(t, b).wait()
            for g in range(groups):
                freq = dot(ahead[:, :BLOCK], hist_buf[b, pl.ds(g * BLOCK, BLOCK), cols(t)])
                if g == groups - 1:
                    last_freq[t, b] = freq
                else:
                    data_freq[b, g] = freq
            for r in range(0, HALF, STEP):
                real = imag = None
                upper, lower = pl.ds(r, STEP), pl.ds(HALF + r, STEP)
                for g in range(groups):
                    data = last_freq.at[t, b] if g == groups - 1 else data_freq.at[b, g]
                    tc, ts = taps_freq[g, upper, :], taps_freq[g, lower, :]
                    dc, ds = data[upper, :], data[lower, :]
                    re = tc * dc + ts * ds
                    im = tc * ds - ts * dc
                    real = re if real is None else real + re
                    imag = im if imag is None else imag + im
                mixed[b, upper, :] = real.astype(jnp.bfloat16)
                mixed[b, lower, :] = imag.astype(jnp.bfloat16)
        for b in range(seqs):
            partial[t, b] = dot(back[...], mixed[b])

    def corner_part(p):
        lane = pl.ds(p * width, width)
        taps_freq[0, :, lane] = dot(ahead[:, BLOCK:], taps_buf[pl.ds(rows, NEW), lane])
        for b in range(seqs):
            for r in range(0, HALF, STEP):
                upper, lower = pl.ds(r, STEP), pl.ds(HALF + r, STEP)
                tc, ts = taps_freq[0, upper, lane], taps_freq[0, lower, lane]
                dc, ds = last_freq[0, b, upper, lane], last_freq[0, b, lower, lane]
                mixed[b, upper, lane] = (tc * dc + ts * ds).astype(jnp.bfloat16)
                mixed[b, lower, lane] = (tc * ds - ts * dc).astype(jnp.bfloat16)
        for b in range(seqs):
            partial[0, b, :, lane] += dot(back[...], mixed[b, :, lane])

    def skip_part(t):
        for b in range(seqs):
            newest = hist_buf[b, pl.ds(rows - NEW, NEW), cols(t)].astype(jnp.float32)
            partial[t, b] += skip_buf[:, cols(t)] * newest

    def pack(t):
        low = lax.rem(lax.broadcasted_iota(jnp.int32, (NEW, lanes), 0), 8) < 4
        evens, odds = [], []
        for b in range(0, seqs, 2):
            first, second = partial[t, b], partial[t, b + 1]
            evens.append(jnp.where(low, first, pltpu.roll(second, 4, 0)))
            odds.append(jnp.where(low, pltpu.roll(first, NEW - 4, 0), second))
        for d in range(count):
            source = odds if d % 2 else evens
            at = d // 2 * 8
            piece = jnp.concatenate([source[0][at : at + 8], source[1][at : at + 8]], axis=0)
            send_buf[d, :, cols(t)] = piece.astype(jnp.bfloat16)

    def send(d):
        return pltpu.make_async_remote_copy(
            src_ref=send_buf.at[d],
            dst_ref=recv_buf.at[me],
            send_sem=send_sem.at[d],
            recv_sem=recv_sem.at[me],
            device_id={"hist": d},
            device_id_type=MESH,
        )

    def arrival(d):
        return pltpu.make_async_remote_copy(
            src_ref=send_buf.at[d],
            dst_ref=recv_buf.at[d],
            send_sem=send_sem.at[d],
            recv_sem=recv_sem.at[d],
            device_id={"hist": d},
            device_id_type=MESH,
        )

    def greet():
        for other in range(1, count):
            told = jnp.logical_and(me > 0, me < other)
            if other in beside:
                told = me < other

            @pl.when(told)
            def _():
                pl.semaphore_signal(barrier, inc=1, device_id={"hist": other}, device_id_type=MESH)

        for other in range(cores - 1):

            @pl.when(jnp.logical_and(core == other, jnp.logical_and(me > 0, me < last)))
            def _():
                pl.semaphore_signal(
                    barrier,
                    inc=1,
                    device_id={"hist": lax.rem(me + 1, count), "seq": sender},
                    device_id_type=MESH,
                )

    def tell_ready(other):
        pl.semaphore_signal(
            ready_sem.at[me], inc=1, device_id={"hist": other}, device_id_type=MESH
        )

    def meet():
        others = jnp.where(jnp.logical_and(core == sender, me > 1), cores - 1, 0)
        pl.semaphore_wait(barrier, me - jnp.where(is_beside, 0, 1) + others)

        for target in range(cores):

            @pl.when(sends_rim(target))
            def _():
                for p in range(parts):
                    rim(p, target).start()

        @pl.when(is_beside)
        def _():
            tell_ready(0)

        for other in range(1, count - 1):

            @pl.when(other < me)
            def _():
                tell_ready(other)

    smalls[0].start()
    smalls[1].start()
    taps_copy(0).start()
    for b in range(seqs // 2):
        hist_copy(0, b).start()

    with jax.named_scope("greet"):
        greet()

    with jax.named_scope("meet"):

        @pl.when(me != 0)
        def _():
            meet()

    with jax.named_scope("loads"):
        for b in range(seqs // 2, seqs):
            hist_copy(0, b).start()
        for t in range(1, tiles):
            taps_copy(t).start()
            for b in range(seqs):
                hist_copy(t, b).start()
        for copy in smalls[2:]:
            copy.start()

    with jax.named_scope("ahead"):
        smalls[0].wait()
        smalls[1].wait()
    @pl.loop(0, tiles)
    def _(t):
        with jax.named_scope("main"):
            main_part(t)

    @pl.when(me != last)
    def _():
        for p in range(parts):
            with jax.named_scope("rim_wait"):
                rim(p, 0).wait_recv()
            with jax.named_scope("corner"):
                corner_part(p)

    with jax.named_scope("skip"):
        smalls[2].wait()
        smalls[3].wait()

        @pl.when(me == last)
        def _():
            for t in range(tiles):
                skip_part(t)

    with jax.named_scope("pack"):
        for t in range(tiles):
            pack(t)

    def ready(d):
        with jax.named_scope("ready"):

            @pl.when(me < d)
            def _():
                pl.semaphore_wait(ready_sem.at[d], 1)

    def relay(d):
        if d in relays:

            @pl.when(me == relays[d])
            def _():
                pl.semaphore_signal(zero_sem, inc=1, device_id={"hist": d}, device_id_type=MESH)

    is_late = me >= count - 2
    singly = 2

    @pl.when(is_beside)
    def _():
        send(0).start()

    @pl.when(is_late)
    def _():
        send(0).wait_send()

    is_between = jnp.logical_not(jnp.logical_or(is_beside, me == 0))

    first = range(1, 5)
    held_from = count - 4
    is_held = me >= held_from

    for d in range(1, held_from):
        early = jnp.logical_and(is_between, d < me)
        if d not in first:
            early = jnp.logical_and(early, jnp.logical_not(is_held))

        @pl.when(early)
        def _():
            send(d).start()

    with jax.named_scope("zero"):

        @pl.when(is_between)
        def _():
            pl.semaphore_wait(zero_sem, 1)
            tell_ready(0)
            send(0).start()

    def arrive(d):
        with jax.named_scope("arrive"):
            arrival(d).wait_recv()

    for d in first:
        ready(d)
        relay(d)

        @pl.when(jnp.logical_and(me != d, jnp.logical_not(is_between)))
        def _():
            send(d).start()

        if d < singly:

            @pl.when(is_late)
            def _():
                send(d).wait_send()

    @pl.when(me == last)
    def _():
        for d in range(held_from, last):
            send(d).start()
        arrive(last - 1)

    @pl.when(jnp.logical_and(is_held, me != last))
    def _():
        arrive(last)

    for d in range(first[-1] + 1, count):
        now = me != d
        if d in tail:
            now = jnp.logical_or(me == 0, me > d)
        if d >= held_from:
            now = jnp.logical_and(now, me != last)
        else:
            sent = jnp.logical_and(jnp.logical_and(is_between, jnp.logical_not(is_held)), d < me)
            now = jnp.logical_and(now, jnp.logical_not(sent))

        @pl.when(jnp.logical_and(now, me < d))
        def _():
            ready(d)

        relay(d)

        @pl.when(now)
        def _():
            send(d).start()

    @pl.when(me != last - 2)
    def _():
        arrive(last - 2)

    for d in tail:

        @pl.when(jnp.logical_and(me > 0, me < d))
        def _():
            ready(d)
            send(d).start()

    gate = jnp.concatenate([gate_buf[b].astype(jnp.float32) for b in range(seqs)], axis=0)
    recv_buf[me] = send_buf[me]
    total = None
    for d in range(count):
        due = me != d
        if d == last - 1:
            due = jnp.logical_and(due, me != last)
        if d == last:
            due = me < held_from
        if d != last - 2:

            @pl.when(due)
            def _():
                arrive(d)

        value = recv_buf[d].astype(jnp.float32)
        total = value if total is None else total + value
    result = (gate * total).astype(jnp.bfloat16)
    for b in range(seqs):
        output[b] = result[b * own : (b + 1) * own]

    with jax.named_scope("drain"):

        for target in range(cores):

            @pl.when(sends_rim(target))
            def _():
                for p in range(parts):
                    rim(p, target).wait_send()

        for d in range(count):
            left = me != d
            if d < singly:
                left = jnp.logical_and(left, jnp.logical_not(is_late))

            @pl.when(left)
            def _():
                send(d).wait_send()


def body(history, filter_taps, skip_gain, gate_values):
    count = lax.axis_size("hist")
    seqs, rows, channels = history.shape
    own = gate_values.shape[1]
    lanes = min(512, channels)
    tiles = channels // lanes
    parts = max(channels // 256, 1)
    groups = rows // BLOCK
    cores = lax.axis_size("seq")
    ahead, back = tables()
    anywhere = pl.BlockSpec(memory_space=pl.ANY)
    f32, bf16 = jnp.float32, jnp.bfloat16
    return pl.pallas_call(
        functools.partial(kernel, lanes, parts),
        out_shape=pltpu.VMEM((seqs, own, channels), bf16),
        in_specs=[anywhere] * 6,
        out_specs=pl.BlockSpec(memory_space=pltpu.VMEM),
        scratch_shapes=[
            pltpu.VMEM((seqs, rows, channels), bf16),
            pltpu.VMEM((rows + NEW, channels), bf16),
            pltpu.VMEM(ahead.shape, bf16),
            pltpu.VMEM(back.shape, bf16),
            pltpu.VMEM((groups, LENGTH, lanes), f32),
            pltpu.VMEM((seqs, groups - 1, LENGTH, lanes), f32),
            pltpu.VMEM((tiles, seqs, LENGTH, lanes), f32),
            pltpu.VMEM((seqs, LENGTH, lanes), bf16),
            pltpu.VMEM((tiles, seqs, NEW, lanes), f32),
            pltpu.VMEM((count, seqs * own, channels), bf16),
            pltpu.VMEM((count, seqs * own, channels), bf16),
            pltpu.VMEM((seqs, own, channels), bf16),
            pltpu.VMEM((1, channels), f32),
            pltpu.SemaphoreType.DMA((tiles, seqs)),
            pltpu.SemaphoreType.DMA((tiles,)),
            pltpu.SemaphoreType.DMA((4,)),
            pltpu.SemaphoreType.DMA((parts, cores)),
            pltpu.SemaphoreType.DMA((parts,)),
            pltpu.SemaphoreType.DMA((count,)),
            pltpu.SemaphoreType.DMA((count,)),
            pltpu.SemaphoreType.REGULAR((count,)),
            pltpu.SemaphoreType.REGULAR,
        ],
        compiler_params=pltpu.CompilerParams(collective_id=0, has_side_effects=True),
        name="hyena_window",
    )(history, filter_taps, skip_gain.reshape(1, channels), gate_values, ahead, back)


def solution(mesh):
    placed = (
        P(("grp", "seq"), "hist", "chan"),
        P(("grp", "hist"), "chan"),
        P(("grp", "chan")),
        P(("grp", "seq"), "hist", "chan"),
    )
    return jax.shard_map(
        body,
        mesh=mesh,
        in_specs=placed,
        out_specs=P(("grp", "seq"), "hist", "chan"),
        check_vma=False,
    )
```

```python
import functools

import jax
import jax.numpy as jnp
import numpy as np
from jax import lax
from jax.experimental import pallas as pl
from jax.experimental.pallas import tpu as pltpu
from jax.sharding import PartitionSpec as P

NEW = 64
BLOCK = 128
LENGTH = BLOCK + NEW
HALF = LENGTH // 2
STEP = 16
MESH = pl.DeviceIdType.MESH


def tables():
    freqs = np.arange(HALF) + 0.5
    angle = 2.0 * np.pi / LENGTH * np.outer(freqs, np.arange(LENGTH))
    ahead = np.concatenate([np.cos(angle), np.sin(angle)], axis=0)
    lags = NEW - 1 - np.arange(NEW)
    angle = 2.0 * np.pi / LENGTH * np.outer(lags, freqs)
    back = np.concatenate([np.cos(angle), -np.sin(angle)], axis=1) * (2.0 / LENGTH)
    return jnp.asarray(ahead, jnp.bfloat16), jnp.asarray(back, jnp.bfloat16)


def dot(a, b):
    return jnp.dot(a, b, preferred_element_type=jnp.float32)


def kernel(
    lanes,
    parts,
    history,
    filter_taps,
    skip_gain,
    gate_values,
    ahead_table,
    back_table,
    output,
    hist_buf,
    taps_buf,
    ahead,
    back,
    taps_freq,
    data_freq,
    last_freq,
    mixed,
    partial,
    send_buf,
    recv_buf,
    gate_buf,
    skip_buf,
    hist_sem,
    taps_sem,
    small_sem,
    rim_send,
    rim_recv,
    send_sem,
    recv_sem,
    ready_sem,
    zero_sem,
):
    count = lax.axis_size("hist")
    me = lax.axis_index("hist")
    seqs, rows, channels = hist_buf.shape
    own = NEW // count
    tiles = channels // lanes
    groups = rows // BLOCK
    last = count - 1

    beside = [i for i in range(1, count) if i <= 3 or i >= count - 3]
    relays = {i: 3 if i < 8 else 7 if i < 12 else 1 for i in range(1, count) if i not in beside}
    tail = range(count - 3, count)

    def is_in(group):
        found = me == group[0]
        for i in group[1:]:
            found = jnp.logical_or(found, me == i)
        return found

    is_beside = is_in(beside)

    def cols(t):
        if not isinstance(t, int):
            return pl.ds(pl.multiple_of(t * lanes, lanes), lanes)
        return pl.ds(t * lanes, lanes)

    def taps_copy(t):
        return pltpu.make_async_copy(
            filter_taps.at[:, cols(t)], taps_buf.at[pl.ds(0, rows), cols(t)], taps_sem.at[t]
        )

    def hist_copy(t, b):
        return pltpu.make_async_copy(
            history.at[b, :, cols(t)], hist_buf.at[b, :, cols(t)], hist_sem.at[t, b]
        )

    smalls = [
        pltpu.make_async_copy(source, target, small_sem.at[i])
        for i, (source, target) in enumerate(
            [
                (ahead_table, ahead),
                (back_table, back),
                (skip_gain, skip_buf),
                (gate_values, gate_buf),
            ]
        )
    ]
    barrier = pltpu.get_barrier_semaphore()

    cores = lax.axis_size("seq")
    core = lax.axis_index("seq")
    sender = cores - 1
    width = channels // parts

    def rim(p, target):
        lane = pl.ds(p * width, width)
        return pltpu.make_async_remote_copy(
            src_ref=filter_taps.at[pl.ds(0, NEW), lane],
            dst_ref=taps_buf.at[pl.ds(rows, NEW), lane],
            send_sem=rim_send.at[p, target],
            recv_sem=rim_recv.at[p],
            device_id={"hist": lax.rem(me + last, count), "seq": target},
            device_id_type=MESH,
        )

    def sends_rim(target):
        return jnp.where(me > 1, core == sender, jnp.logical_and(me == 1, core == target))

    def main_part(t):
        taps_copy(t).wait()
        for g in range(groups):
            span = BLOCK if g == groups - 1 else LENGTH
            taps_freq[g] = dot(ahead[:, :span], taps_buf[pl.ds(g * BLOCK, span), cols(t)])
        for b in range(seqs):
            hist_copy(t, b).wait()
            for g in range(groups):
                freq = dot(ahead[:, :BLOCK], hist_buf[b, pl.ds(g * BLOCK, BLOCK), cols(t)])
                if g == groups - 1:
                    last_freq[t, b] = freq
                else:
                    data_freq[b, g] = freq
            for r in range(0, HALF, STEP):
                real = imag = None
                upper, lower = pl.ds(r, STEP), pl.ds(HALF + r, STEP)
                for g in range(groups):
                    data = last_freq.at[t, b] if g == groups - 1 else data_freq.at[b, g]
                    tc, ts = taps_freq[g, upper, :], taps_freq[g, lower, :]
                    dc, ds = data[upper, :], data[lower, :]
                    re = tc * dc + ts * ds
                    im = tc * ds - ts * dc
                    real = re if real is None else real + re
                    imag = im if imag is None else imag + im
                mixed[b, upper, :] = real.astype(jnp.bfloat16)
                mixed[b, lower, :] = imag.astype(jnp.bfloat16)
        for b in range(seqs):
            partial[t, b] = dot(back[...], mixed[b])

    def corner_part(p):
        lane = pl.ds(p * width, width)
        taps_freq[0, :, lane] = dot(ahead[:, BLOCK:], taps_buf[pl.ds(rows, NEW), lane])
        for b in range(seqs):
            for r in range(0, HALF, STEP):
                upper, lower = pl.ds(r, STEP), pl.ds(HALF + r, STEP)
                tc, ts = taps_freq[0, upper, lane], taps_freq[0, lower, lane]
                dc, ds = last_freq[0, b, upper, lane], last_freq[0, b, lower, lane]
                mixed[b, upper, lane] = (tc * dc + ts * ds).astype(jnp.bfloat16)
                mixed[b, lower, lane] = (tc * ds - ts * dc).astype(jnp.bfloat16)
        for b in range(seqs):
            partial[0, b, :, lane] += dot(back[...], mixed[b, :, lane])

    def skip_part(t):
        for b in range(seqs):
            newest = hist_buf[b, pl.ds(rows - NEW, NEW), cols(t)].astype(jnp.float32)
            partial[t, b] += skip_buf[:, cols(t)] * newest

    def pack(t):
        low = lax.rem(lax.broadcasted_iota(jnp.int32, (NEW, lanes), 0), 8) < 4
        evens, odds = [], []
        for b in range(0, seqs, 2):
            first, second = partial[t, b], partial[t, b + 1]
            evens.append(jnp.where(low, first, pltpu.roll(second, 4, 0)))
            odds.append(jnp.where(low, pltpu.roll(first, NEW - 4, 0), second))
        for d in range(count):
            source = odds if d % 2 else evens
            at = d // 2 * 8
            piece = jnp.concatenate([source[0][at : at + 8], source[1][at : at + 8]], axis=0)
            send_buf[d, :, cols(t)] = piece.astype(jnp.bfloat16)

    last_early = count - 5
    singles = 2

    def send(d):
        return pltpu.make_async_remote_copy(
            src_ref=send_buf.at[d],
            dst_ref=recv_buf.at[me],
            send_sem=send_sem.at[min(d, singles)],
            recv_sem=recv_sem.at[jnp.maximum(me - last_early, 0)],
            device_id={"hist": d},
            device_id_type=MESH,
        )

    def arrival(d, n=1):
        return pltpu.make_async_remote_copy(
            src_ref=send_buf.at[pl.ds(d, n)],
            dst_ref=recv_buf.at[pl.ds(d, n)],
            send_sem=send_sem.at[min(d, singles)],
            recv_sem=recv_sem.at[max(d - last_early, 0)],
            device_id={"hist": d},
            device_id_type=MESH,
        )

    def greet():
        for other in range(1, count):
            told = jnp.logical_and(me > 0, me < other)
            if other in beside:
                told = me < other

            @pl.when(told)
            def _():
                pl.semaphore_signal(barrier, inc=1, device_id={"hist": other}, device_id_type=MESH)

        for other in range(cores - 1):

            @pl.when(jnp.logical_and(core == other, jnp.logical_and(me > 0, me < last)))
            def _():
                pl.semaphore_signal(
                    barrier,
                    inc=1,
                    device_id={"hist": lax.rem(me + 1, count), "seq": sender},
                    device_id_type=MESH,
                )

    def tell_ready(other):
        pl.semaphore_signal(
            ready_sem.at[me], inc=1, device_id={"hist": other}, device_id_type=MESH
        )

    def meet():
        others = jnp.where(jnp.logical_and(core == sender, me > 1), cores - 1, 0)
        pl.semaphore_wait(barrier, me - jnp.where(is_beside, 0, 1) + others)

        for target in range(cores):

            @pl.when(sends_rim(target))
            def _():
                for p in range(parts):
                    rim(p, target).start()

        @pl.when(core == sender)
        def _():
            load()

        @pl.when(is_beside)
        def _():
            tell_ready(0)

        for other in range(1, count - 1):

            @pl.when(other < me)
            def _():
                tell_ready(other)

    def load():
        smalls[0].start()
        for t in range(tiles):
            taps_copy(t).start()
            for b in range(seqs):
                hist_copy(t, b).start()
        for copy in smalls[1:]:
            copy.start()

    @pl.when(jnp.logical_or(core != sender, me == 0))
    def _():
        load()

    with jax.named_scope("greet"):
        greet()

    with jax.named_scope("meet"):

        @pl.when(me != 0)
        def _():
            meet()

    with jax.named_scope("ahead"):
        smalls[0].wait()
        smalls[1].wait()
    @pl.loop(0, tiles)
    def _(t):
        with jax.named_scope("main"):
            main_part(t)

    @pl.when(me != last)
    def _():
        for p in range(parts):
            with jax.named_scope("rim_wait"):
                rim(p, 0).wait_recv()
            with jax.named_scope("corner"):
                corner_part(p)

    with jax.named_scope("skip"):
        smalls[2].wait()
        smalls[3].wait()

        @pl.when(me == last)
        def _():
            for t in range(tiles):
                skip_part(t)

    with jax.named_scope("pack"):
        for t in range(tiles):
            pack(t)

    def ready(d):
        with jax.named_scope("ready"):

            @pl.when(me < d)
            def _():
                pl.semaphore_wait(ready_sem.at[d], 1)

    def relay(d):
        if d in relays:

            @pl.when(me == relays[d])
            def _():
                pl.semaphore_signal(zero_sem, inc=1, device_id={"hist": d}, device_id_type=MESH)

    is_late = me >= count - 2
    singly = 2

    @pl.when(is_beside)
    def _():
        send(0).start()

    @pl.when(is_late)
    def _():
        send(0).wait_send()

    is_between = jnp.logical_not(jnp.logical_or(is_beside, me == 0))

    first = range(1, 5)
    held_from = count - 4
    is_held = me >= held_from

    for d in range(1, held_from):
        early = jnp.logical_and(is_between, d < me)
        if d not in first:
            early = jnp.logical_and(early, jnp.logical_not(is_held))

        @pl.when(early)
        def _():
            send(d).start()

    with jax.named_scope("zero"):

        @pl.when(is_between)
        def _():
            pl.semaphore_wait(zero_sem, 1)
            tell_ready(0)
            send(0).start()

    def arrive(d):
        with jax.named_scope("arrive"):
            arrival(d).wait_recv()

    for d in first:
        ready(d)
        relay(d)

        now = jnp.logical_and(me != d, jnp.logical_not(is_between))
        if d == first[-1]:
            now = jnp.logical_and(now, me != held_from + 1)

        @pl.when(now)
        def _():
            send(d).start()

        if d < singly:

            @pl.when(is_late)
            def _():
                send(d).wait_send()

    @pl.when(me == last)
    def _():
        for d in range(held_from, last):
            send(d).start()
        arrive(last - 1)

    @pl.when(jnp.logical_and(is_held, me != last))
    def _():
        arrive(last)

    @pl.when(me == held_from + 1)
    def _():
        send(first[-1]).start()

    for d in range(first[-1] + 1, count):
        now = me != d
        if d in tail:
            now = jnp.logical_or(me == 0, me > d)
        if d >= held_from:
            now = jnp.logical_and(now, me != last)
        else:
            sent = jnp.logical_and(jnp.logical_and(is_between, jnp.logical_not(is_held)), d < me)
            now = jnp.logical_and(now, jnp.logical_not(sent))

        @pl.when(jnp.logical_and(now, me < d))
        def _():
            ready(d)

        relay(d)

        @pl.when(now)
        def _():
            send(d).start()

    @pl.when(me == 1)
    def _():
        arrive(held_from)

    @pl.when(jnp.logical_and(me != 1, me != last - 2))
    def _():
        arrive(last - 2)

    for d in tail:

        @pl.when(jnp.logical_and(me > 0, me < d))
        def _():
            ready(d)
            send(d).start()

    gate = jnp.concatenate([gate_buf[b].astype(jnp.float32) for b in range(seqs)], axis=0)
    recv_buf[me] = send_buf[me]
    total = None
    with jax.named_scope("early"):
        for missing in range(2):

            @pl.when((me <= last_early) == bool(missing))
            def _():
                arrival(0, last_early + 1 - missing).wait_recv()

    for d in range(count):
        due = me != d
        if d == held_from:
            due = jnp.logical_and(due, me != 1)
        if d == last - 2:
            due = me == 1
        if d == last - 1:
            due = jnp.logical_and(due, me != last)
        if d == last:
            due = me < held_from
        if d > last_early:

            @pl.when(due)
            def _():
                arrive(d)

        value = recv_buf[d].astype(jnp.float32)
        total = value if total is None else total + value
    result = (gate * total).astype(jnp.bfloat16)
    for b in range(seqs):
        output[b] = result[b * own : (b + 1) * own]

    with jax.named_scope("drain"):

        for target in range(cores):

            @pl.when(sends_rim(target))
            def _():
                for p in range(parts):
                    rim(p, target).wait_send()

        for d in range(singles):
            left = me != d
            if d < singly:
                left = jnp.logical_and(left, jnp.logical_not(is_late))

            @pl.when(left)
            def _():
                send(d).wait_send()

        for missing in range(2):

            @pl.when((me >= singles) == bool(missing))
            def _():
                arrival(singles, count - singles - missing).wait_send()


def body(history, filter_taps, skip_gain, gate_values):
    count = lax.axis_size("hist")
    seqs, rows, channels = history.shape
    own = gate_values.shape[1]
    lanes = min(512, channels)
    tiles = channels // lanes
    parts = max(channels // 256, 1)
    groups = rows // BLOCK
    cores = lax.axis_size("seq")
    ahead, back = tables()
    anywhere = pl.BlockSpec(memory_space=pl.ANY)
    f32, bf16 = jnp.float32, jnp.bfloat16
    return pl.pallas_call(
        functools.partial(kernel, lanes, parts),
        out_shape=pltpu.VMEM((seqs, own, channels), bf16),
        in_specs=[anywhere] * 6,
        out_specs=pl.BlockSpec(memory_space=pltpu.VMEM),
        scratch_shapes=[
            pltpu.VMEM((seqs, rows, channels), bf16),
            pltpu.VMEM((rows + NEW, channels), bf16),
            pltpu.VMEM(ahead.shape, bf16),
            pltpu.VMEM(back.shape, bf16),
            pltpu.VMEM((groups, LENGTH, lanes), f32),
            pltpu.VMEM((seqs, groups - 1, LENGTH, lanes), f32),
            pltpu.VMEM((tiles, seqs, LENGTH, lanes), f32),
            pltpu.VMEM((seqs, LENGTH, lanes), bf16),
            pltpu.VMEM((tiles, seqs, NEW, lanes), f32),
            pltpu.VMEM((count, seqs * own, channels), bf16),
            pltpu.VMEM((count, seqs * own, channels), bf16),
            pltpu.VMEM((seqs, own, channels), bf16),
            pltpu.VMEM((1, channels), f32),
            pltpu.SemaphoreType.DMA((tiles, seqs)),
            pltpu.SemaphoreType.DMA((tiles,)),
            pltpu.SemaphoreType.DMA((4,)),
            pltpu.SemaphoreType.DMA((parts, cores)),
            pltpu.SemaphoreType.DMA((parts,)),
            pltpu.SemaphoreType.DMA((3,)),
            pltpu.SemaphoreType.DMA((5,)),
            pltpu.SemaphoreType.REGULAR((count,)),
            pltpu.SemaphoreType.REGULAR,
        ],
        compiler_params=pltpu.CompilerParams(collective_id=0, has_side_effects=True),
        name="hyena_window",
    )(history, filter_taps, skip_gain.reshape(1, channels), gate_values, ahead, back)


def solution(mesh):
    placed = (
        P(("grp", "seq"), "hist", "chan"),
        P(("grp", "hist"), "chan"),
        P(("grp", "chan")),
        P(("grp", "seq"), "hist", "chan"),
    )
    return jax.shard_map(
        body,
        mesh=mesh,
        in_specs=placed,
        out_specs=P(("grp", "seq"), "hist", "chan"),
        check_vma=False,
    )
```

```python
import functools

import jax
import jax.numpy as jnp
import numpy as np
from jax import lax
from jax.experimental import pallas as pl
from jax.experimental.pallas import tpu as pltpu
from jax.sharding import PartitionSpec as P

NEW = 64
BLOCK = 128
LENGTH = BLOCK + NEW
HALF = LENGTH // 2
STEP = 16
MESH = pl.DeviceIdType.MESH


def tables():
    freqs = np.arange(HALF) + 0.5
    angle = 2.0 * np.pi / LENGTH * np.outer(freqs, np.arange(LENGTH))
    ahead = np.concatenate([np.cos(angle), np.sin(angle)], axis=0)
    lags = NEW - 1 - np.arange(NEW)
    angle = 2.0 * np.pi / LENGTH * np.outer(lags, freqs)
    back = np.concatenate([np.cos(angle), -np.sin(angle)], axis=1) * (2.0 / LENGTH)
    return jnp.asarray(ahead, jnp.bfloat16), jnp.asarray(back, jnp.bfloat16)


def dot(a, b):
    return jnp.dot(a, b, preferred_element_type=jnp.float32)


def kernel(
    lanes,
    parts,
    history,
    filter_taps,
    skip_gain,
    gate_values,
    ahead_table,
    back_table,
    output,
    hist_buf,
    taps_buf,
    ahead,
    back,
    taps_freq,
    data_freq,
    last_freq,
    mixed,
    partial,
    send_buf,
    recv_buf,
    gate_buf,
    skip_buf,
    hist_sem,
    taps_sem,
    small_sem,
    rim_send,
    rim_recv,
    send_sem,
    recv_sem,
    ready_sem,
    zero_sem,
):
    count = lax.axis_size("hist")
    me = lax.axis_index("hist")
    seqs, rows, channels = hist_buf.shape
    own = NEW // count
    tiles = channels // lanes
    groups = rows // BLOCK
    last = count - 1

    beside = [i for i in range(1, count) if i <= 3 or i >= count - 3]
    relays = {i: 3 if i < 8 else 7 if i < 12 else 1 for i in range(1, count) if i not in beside}
    tail = range(count - 3, count)

    def is_in(group):
        found = me == group[0]
        for i in group[1:]:
            found = jnp.logical_or(found, me == i)
        return found

    is_beside = is_in(beside)

    def cols(t):
        if not isinstance(t, int):
            return pl.ds(pl.multiple_of(t * lanes, lanes), lanes)
        return pl.ds(t * lanes, lanes)

    def taps_copy(t):
        return pltpu.make_async_copy(
            filter_taps.at[:, cols(t)], taps_buf.at[pl.ds(0, rows), cols(t)], taps_sem.at[t]
        )

    def hist_copy(t, b):
        return pltpu.make_async_copy(
            history.at[b, :, cols(t)], hist_buf.at[b, :, cols(t)], hist_sem.at[t, b]
        )

    smalls = [
        pltpu.make_async_copy(source, target, small_sem.at[i])
        for i, (source, target) in enumerate(
            [
                (ahead_table, ahead),
                (back_table, back),
                (skip_gain, skip_buf),
                (gate_values, gate_buf),
            ]
        )
    ]
    barrier = pltpu.get_barrier_semaphore()

    cores = lax.axis_size("seq")
    core = lax.axis_index("seq")
    sender = cores - 1
    width = channels // parts

    def rim(p, target):
        lane = pl.ds(p * width, width)
        return pltpu.make_async_remote_copy(
            src_ref=filter_taps.at[pl.ds(0, NEW), lane],
            dst_ref=taps_buf.at[pl.ds(rows, NEW), lane],
            send_sem=rim_send.at[p, target],
            recv_sem=rim_recv.at[p],
            device_id={"hist": lax.rem(me + last, count), "seq": target},
            device_id_type=MESH,
        )

    def sends_rim(target):
        return jnp.where(me > 1, core == sender, jnp.logical_and(me == 1, core == target))

    def main_part(t):
        taps_copy(t).wait()
        for g in range(groups):
            span = BLOCK if g == groups - 1 else LENGTH
            taps_freq[g] = dot(ahead[:, :span], taps_buf[pl.ds(g * BLOCK, span), cols(t)])
        for b in range(seqs):
            hist_copy(t, b).wait()
            for g in range(groups):
                freq = dot(ahead[:, :BLOCK], hist_buf[b, pl.ds(g * BLOCK, BLOCK), cols(t)])
                if g == groups - 1:
                    last_freq[t, b] = freq
                else:
                    data_freq[b, g] = freq
            for r in range(0, HALF, STEP):
                real = imag = None
                upper, lower = pl.ds(r, STEP), pl.ds(HALF + r, STEP)
                for g in range(groups):
                    data = last_freq.at[t, b] if g == groups - 1 else data_freq.at[b, g]
                    tc, ts = taps_freq[g, upper, :], taps_freq[g, lower, :]
                    dc, ds = data[upper, :], data[lower, :]
                    re = tc * dc + ts * ds
                    im = tc * ds - ts * dc
                    real = re if real is None else real + re
                    imag = im if imag is None else imag + im
                mixed[b, upper, :] = real.astype(jnp.bfloat16)
                mixed[b, lower, :] = imag.astype(jnp.bfloat16)
        for b in range(seqs):
            partial[t, b] = dot(back[...], mixed[b])

    def corner_part(p):
        lane = pl.ds(p * width, width)
        taps_freq[0, :, lane] = dot(ahead[:, BLOCK:], taps_buf[pl.ds(rows, NEW), lane])
        for b in range(seqs):
            for r in range(0, HALF, STEP):
                upper, lower = pl.ds(r, STEP), pl.ds(HALF + r, STEP)
                tc, ts = taps_freq[0, upper, lane], taps_freq[0, lower, lane]
                dc, ds = last_freq[0, b, upper, lane], last_freq[0, b, lower, lane]
                mixed[b, upper, lane] = (tc * dc + ts * ds).astype(jnp.bfloat16)
                mixed[b, lower, lane] = (tc * ds - ts * dc).astype(jnp.bfloat16)
        for b in range(seqs):
            partial[0, b, :, lane] += dot(back[...], mixed[b, :, lane])

    def skip_part(t):
        for b in range(seqs):
            newest = hist_buf[b, pl.ds(rows - NEW, NEW), cols(t)].astype(jnp.float32)
            partial[t, b] += skip_buf[:, cols(t)] * newest

    def pack(t):
        low = lax.rem(lax.broadcasted_iota(jnp.int32, (NEW, lanes), 0), 8) < 4
        evens, odds = [], []
        for b in range(0, seqs, 2):
            first, second = partial[t, b], partial[t, b + 1]
            evens.append(jnp.where(low, first, pltpu.roll(second, 4, 0)))
            odds.append(jnp.where(low, pltpu.roll(first, NEW - 4, 0), second))
        for d in range(count):
            source = odds if d % 2 else evens
            at = d // 2 * 8
            piece = jnp.concatenate([source[0][at : at + 8], source[1][at : at + 8]], axis=0)
            send_buf[d, :, cols(t)] = piece.astype(jnp.bfloat16)

    last_early = count - 5
    singles = 2

    def send(d):
        return pltpu.make_async_remote_copy(
            src_ref=send_buf.at[d],
            dst_ref=recv_buf.at[me],
            send_sem=send_sem.at[min(d, singles)],
            recv_sem=recv_sem.at[jnp.maximum(me - last_early, 0)],
            device_id={"hist": d},
            device_id_type=MESH,
        )

    def arrival(d, n=1):
        return pltpu.make_async_remote_copy(
            src_ref=send_buf.at[pl.ds(d, n)],
            dst_ref=recv_buf.at[pl.ds(d, n)],
            send_sem=send_sem.at[min(d, singles)],
            recv_sem=recv_sem.at[max(d - last_early, 0)],
            device_id={"hist": d},
            device_id_type=MESH,
        )

    def greet():
        for other in range(1, count):
            told = jnp.logical_and(me > 0, me < other)
            if other in beside:
                told = me < other

            @pl.when(told)
            def _():
                pl.semaphore_signal(barrier, inc=1, device_id={"hist": other}, device_id_type=MESH)

        for other in range(cores - 1):

            @pl.when(jnp.logical_and(core == other, jnp.logical_and(me > 0, me < last)))
            def _():
                pl.semaphore_signal(
                    barrier,
                    inc=1,
                    device_id={"hist": lax.rem(me + 1, count), "seq": sender},
                    device_id_type=MESH,
                )

    def tell_ready(other):
        pl.semaphore_signal(
            ready_sem.at[me], inc=1, device_id={"hist": other}, device_id_type=MESH
        )

    def meet():
        others = jnp.where(jnp.logical_and(core == sender, me > 1), cores - 1, 0)
        pl.semaphore_wait(barrier, me - jnp.where(is_beside, 0, 1) + others)

        for target in range(cores):

            @pl.when(sends_rim(target))
            def _():
                for p in range(parts):
                    rim(p, target).start()

        @pl.when(core == sender)
        def _():
            load()

        @pl.when(is_beside)
        def _():
            tell_ready(0)

        for other in range(1, count - 1):

            @pl.when(other < me)
            def _():
                tell_ready(other)

    def load():
        smalls[0].start()
        for t in range(tiles):
            taps_copy(t).start()
            for b in range(seqs):
                hist_copy(t, b).start()
        for copy in smalls[1:]:
            copy.start()

    @pl.when(jnp.logical_or(core != sender, me == 0))
    def _():
        load()

    with jax.named_scope("greet"):
        greet()

    with jax.named_scope("meet"):

        @pl.when(me != 0)
        def _():
            meet()

    with jax.named_scope("ahead"):
        smalls[0].wait()
        smalls[1].wait()
    @pl.loop(0, tiles)
    def _(t):
        with jax.named_scope("main"):
            main_part(t)

    @pl.when(me != last)
    def _():
        for p in range(parts):
            with jax.named_scope("rim_wait"):
                rim(p, 0).wait_recv()
            with jax.named_scope("corner"):
                corner_part(p)

    with jax.named_scope("skip"):
        smalls[2].wait()
        smalls[3].wait()

        @pl.when(me == last)
        def _():
            for t in range(tiles):
                skip_part(t)

    with jax.named_scope("pack"):
        for t in range(tiles):
            pack(t)

    def ready(d):
        with jax.named_scope("ready"):

            @pl.when(me < d)
            def _():
                pl.semaphore_wait(ready_sem.at[d], 1)

    def relay(d):
        if d in relays:

            @pl.when(me == relays[d])
            def _():
                pl.semaphore_signal(zero_sem, inc=1, device_id={"hist": d}, device_id_type=MESH)

    is_late = me >= count - 2
    singly = 2

    @pl.when(is_beside)
    def _():
        send(0).start()

    @pl.when(is_late)
    def _():
        send(0).wait_send()

    is_between = jnp.logical_not(jnp.logical_or(is_beside, me == 0))

    first = range(1, 5)
    held_from = count - 4
    is_held = me >= held_from

    for d in range(1, held_from):
        early = jnp.logical_and(is_between, d < me)
        if d not in first:
            early = jnp.logical_and(early, jnp.logical_not(is_held))

        @pl.when(early)
        def _():
            send(d).start()

    with jax.named_scope("zero"):

        @pl.when(is_between)
        def _():
            pl.semaphore_wait(zero_sem, 1)
            tell_ready(0)
            send(0).start()

    def arrive(d):
        with jax.named_scope("arrive"):
            arrival(d).wait_recv()

    for d in first:
        ready(d)
        relay(d)

        now = jnp.logical_and(me != d, jnp.logical_not(is_between))
        if d == first[-1]:
            now = jnp.logical_and(now, me != held_from + 1)

        @pl.when(now)
        def _():
            send(d).start()

        if d < singly:

            @pl.when(is_late)
            def _():
                send(d).wait_send()

    @pl.when(me == last)
    def _():
        for d in range(held_from, last):
            send(d).start()
        arrive(last - 1)

    @pl.when(jnp.logical_and(is_held, me != last))
    def _():
        arrive(last)

    @pl.when(me == held_from + 1)
    def _():
        send(first[-1]).start()

    for d in range(first[-1] + 1, count):
        now = me != d
        if d in tail:
            now = jnp.logical_or(me == 0, me > d)
        if d >= held_from:
            now = jnp.logical_and(now, me != last)
        else:
            sent = jnp.logical_and(jnp.logical_and(is_between, jnp.logical_not(is_held)), d < me)
            now = jnp.logical_and(now, jnp.logical_not(sent))

        @pl.when(jnp.logical_and(now, me < d))
        def _():
            ready(d)

        relay(d)

        @pl.when(now)
        def _():
            send(d).start()

    @pl.when(me == 1)
    def _():
        arrive(held_from)

    @pl.when(jnp.logical_and(me != 1, me != last - 2))
    def _():
        arrive(last - 2)

    for d in tail:

        @pl.when(jnp.logical_and(me > 0, me < d))
        def _():
            ready(d)
            send(d).start()

    gate = jnp.concatenate([gate_buf[b].astype(jnp.float32) for b in range(seqs)], axis=0)
    recv_buf[me] = send_buf[me]
    total = None
    with jax.named_scope("early"):
        for missing in range(2):

            @pl.when((me <= last_early) == bool(missing))
            def _():
                arrival(0, last_early + 1 - missing).wait_recv()

    for d in range(count):
        due = me != d
        if d == held_from:
            due = jnp.logical_and(due, me != 1)
        if d == last - 2:
            due = me == 1
        if d == last - 1:
            due = jnp.logical_and(due, me != last)
        if d == last:
            due = me < held_from
        if d > last_early:

            @pl.when(due)
            def _():
                arrive(d)

        value = recv_buf[d].astype(jnp.float32)
        total = value if total is None else total + value
    result = (gate * total).astype(jnp.bfloat16)
    for b in range(seqs):
        output[b] = result[b * own : (b + 1) * own]

    with jax.named_scope("drain"):

        for target in range(cores):

            @pl.when(sends_rim(target))
            def _():
                for p in range(parts):
                    rim(p, target).wait_send()

        for d in range(singles):
            left = me != d
            if d < singly:
                left = jnp.logical_and(left, jnp.logical_not(is_late))

            @pl.when(left)
            def _():
                send(d).wait_send()

        for missing in range(2):

            @pl.when((me >= singles) == bool(missing))
            def _():
                arrival(singles, count - singles - missing).wait_send()


def body(history, filter_taps, skip_gain, gate_values):
    count = lax.axis_size("hist")
    seqs, rows, channels = history.shape
    own = gate_values.shape[1]
    lanes = min(512, channels)
    tiles = channels // lanes
    parts = 1
    groups = rows // BLOCK
    cores = lax.axis_size("seq")
    ahead, back = tables()
    anywhere = pl.BlockSpec(memory_space=pl.ANY)
    f32, bf16 = jnp.float32, jnp.bfloat16
    return pl.pallas_call(
        functools.partial(kernel, lanes, parts),
        out_shape=pltpu.VMEM((seqs, own, channels), bf16),
        in_specs=[anywhere] * 6,
        out_specs=pl.BlockSpec(memory_space=pltpu.VMEM),
        scratch_shapes=[
            pltpu.VMEM((seqs, rows, channels), bf16),
            pltpu.VMEM((rows + NEW, channels), bf16),
            pltpu.VMEM(ahead.shape, bf16),
            pltpu.VMEM(back.shape, bf16),
            pltpu.VMEM((groups, LENGTH, lanes), f32),
            pltpu.VMEM((seqs, groups - 1, LENGTH, lanes), f32),
            pltpu.VMEM((tiles, seqs, LENGTH, lanes), f32),
            pltpu.VMEM((seqs, LENGTH, lanes), bf16),
            pltpu.VMEM((tiles, seqs, NEW, lanes), f32),
            pltpu.VMEM((count, seqs * own, channels), bf16),
            pltpu.VMEM((count, seqs * own, channels), bf16),
            pltpu.VMEM((seqs, own, channels), bf16),
            pltpu.VMEM((1, channels), f32),
            pltpu.SemaphoreType.DMA((tiles, seqs)),
            pltpu.SemaphoreType.DMA((tiles,)),
            pltpu.SemaphoreType.DMA((4,)),
            pltpu.SemaphoreType.DMA((parts, cores)),
            pltpu.SemaphoreType.DMA((parts,)),
            pltpu.SemaphoreType.DMA((3,)),
            pltpu.SemaphoreType.DMA((5,)),
            pltpu.SemaphoreType.REGULAR((count,)),
            pltpu.SemaphoreType.REGULAR,
        ],
        compiler_params=pltpu.CompilerParams(collective_id=0, has_side_effects=True),
        name="hyena_window",
    )(history, filter_taps, skip_gain.reshape(1, channels), gate_values, ahead, back)


def solution(mesh):
    placed = (
        P(("grp", "seq"), "hist", "chan"),
        P(("grp", "hist"), "chan"),
        P(("grp", "chan")),
        P(("grp", "seq"), "hist", "chan"),
    )
    return jax.shard_map(
        body,
        mesh=mesh,
        in_specs=placed,
        out_specs=P(("grp", "seq"), "hist", "chan"),
        check_vma=False,
    )
```
